256 devices in a mesh: stn: 4 (over z_hi), chan: 64 (over x, z_lo, y, core).
Axes of the slice: x: 4, y: 4, z: 8 (z_hi: 4, z_lo: 2; z = z_hi * 2 + z_lo), core: 2. Of those that a mesh axis runs over, the one named last changes fastest.
Arguments:
- voltages: bfloat16 [1024, 64, 8, 1024], P('stn', 'chan'), may hold values from -6 to 6
- fir_taps: float32 [8, 8, 1024], replicated, may hold values from -2.5 to 2.5
Outputs:
- visibilities: float32 [4, 64, 2, 1024, 1024], P(None, 'chan', None, 'stn')
The draws below stay inside these ranges and needn't reach their ends.
All inputs are finite; a program needn't handle non-finite values.
Results may differ from the reference program's by a relative error of at most 0.0044.
Values may be sent and summed in bfloat16 or wider, within the bound.
A program may use at most 128 MiB of HBM per device.

```python
import math
import jax
import jax.numpy as jnp
from jax import lax

INPUTS = 1024
SLOTS = 1024
PHASES = 8
TAPS = 8
AVG = 16
FR_DEV = 8
GROUPS = 8


def steps_of(key, dims, shards, smallest, high):
    def one(position, shards_of):
        draws = jax.random.uniform(jax.random.fold_in(jax.random.fold_in(key, 6), position), (shards_of,), jnp.float32, smallest / len(shards), high / len(shards))
        return jnp.repeat(jnp.exp(draws), dims[position] // shards_of).reshape((-1,) + (1,) * (len(dims) - position - 1))

    level = one(*shards[0])
    for cut in shards[1:]:
        level = level * one(*cut)
    return level


def scatter_about(own_key, extent, deviation, bound, cuts=(), held_as=jnp.bfloat16):
    array = deviation * jax.random.normal(own_key, extent, jnp.float32)
    if cuts:
        array = array * steps_of(own_key, extent, cuts, -0.22, 0.18)
    return jnp.clip(array, -bound, bound).astype(held_as)


def setup_inputs(seed: int = 0) -> dict:
    arg_keys = jax.random.split(jax.random.key(seed), 3)
    voltages = scatter_about(arg_keys[0], (INPUTS, GROUPS * PHASES, FR_DEV, SLOTS), 1.0, 6.0, ((0, 4), (1, 64)))
    fir_taps = scatter_about(arg_keys[1], (PHASES, TAPS, SLOTS), 0.35, 2.5, (), jnp.float32)
    return {"voltages": voltages, "fir_taps": fir_taps}


def reference(voltages, fir_taps):
    inputs = voltages.shape[0]
    groups = voltages.shape[1] // PHASES
    frames = groups * FR_DEV
    spectra_count = frames - (TAPS - 1)
    band_count = PHASES // 2
    frame_len = PHASES * SLOTS
    ordered = voltages.reshape(inputs, groups, PHASES, FR_DEV, SLOTS)
    ordered = ordered.transpose(0, 1, 3, 2, 4).reshape(inputs, frames, PHASES, SLOTS)
    phase_ids = jnp.arange(PHASES, dtype=jnp.int32)
    slot_ids = jnp.arange(SLOTS, dtype=jnp.int32)
    turn_ids = (phase_ids[:, None] * slot_ids[None, :]) % frame_len
    angles = turn_ids.astype(jnp.float32) * jnp.float32(-2.0 * math.pi / frame_len)
    twist_re = jnp.cos(angles)
    twist_im = jnp.sin(angles)
    band_ids = jnp.arange(band_count, dtype=jnp.int32)
    band_turns = (phase_ids[:, None] * band_ids[None, :]) % PHASES
    band_angles = band_turns.astype(jnp.float32) * jnp.float32(-2.0 * math.pi / PHASES)
    band_re = jnp.cos(band_angles)
    band_im = jnp.sin(band_angles)
    block_len = math.gcd(inputs, 32)
    highest = lax.Precision.HIGHEST

    def channelise(shard_piece):
        widened = shard_piece.astype(jnp.float32)
        filtered = jnp.zeros((block_len, spectra_count, PHASES, SLOTS), jnp.float32)
        for tap_index in range(TAPS):
            first_row = TAPS - 1 - tap_index
            filtered = filtered + fir_taps[:, tap_index, :] * widened[:, first_row:first_row + spectra_count]
        spectrum = jnp.fft.fft(filtered, axis=-1)
        part_re = spectrum.real
        part_im = spectrum.imag
        branch_re = (part_re * twist_re - part_im * twist_im).astype(jnp.bfloat16)
        branch_im = (part_re * twist_im + part_im * twist_re).astype(jnp.bfloat16)
        branch_re = lax.optimization_barrier(branch_re).astype(jnp.float32)
        branch_im = lax.optimization_barrier(branch_im).astype(jnp.float32)
        einsum_form = 'nspk,pb->nsbk'
        spec_re = jnp.einsum(einsum_form, branch_re, band_re, precision=highest) - jnp.einsum(einsum_form, branch_im, band_im, precision=highest)
        spec_im = jnp.einsum(einsum_form, branch_re, band_im, precision=highest) + jnp.einsum(einsum_form, branch_im, band_re, precision=highest)
        return spec_re.astype(jnp.bfloat16), spec_im.astype(jnp.bfloat16)

    pieces = ordered.reshape(inputs // block_len, block_len, frames, PHASES, SLOTS)
    spec_re, spec_im = lax.map(channelise, pieces)
    spec_re = spec_re.reshape(inputs, spectra_count, band_count, SLOTS)
    spec_im = spec_im.reshape(inputs, spectra_count, band_count, SLOTS)
    subs = SLOTS // AVG
    scaling = 1.0 / (frame_len * AVG * spectra_count)

    def correlate(flat_index):
        band_at = flat_index // subs
        sub_at = flat_index % subs
        zero_at = jnp.int32(0)
        corner = (zero_at, zero_at, band_at.astype(jnp.int32), (sub_at * AVG).astype(jnp.int32))
        sizes = (inputs, spectra_count, 1, AVG)
        left_re = lax.dynamic_slice(spec_re, corner, sizes).reshape(inputs, spectra_count * AVG)
        left_im = lax.dynamic_slice(spec_im, corner, sizes).reshape(inputs, spectra_count * AVG)
        vis_re = jnp.dot(left_re, left_re.T, preferred_element_type=jnp.float32) + jnp.dot(left_im, left_im.T, preferred_element_type=jnp.float32)
        vis_im = jnp.dot(left_im, left_re.T, preferred_element_type=jnp.float32) - jnp.dot(left_re, left_im.T, preferred_element_type=jnp.float32)
        return jnp.stack([vis_re, vis_im]) * scaling

    result = lax.map(correlate, jnp.arange(band_count * subs, dtype=jnp.int32))
    return result.reshape(band_count, subs, 2, inputs, inputs)
```

```python
import math

import jax
import jax.numpy as jnp
import numpy as np
from jax import lax
from jax.experimental import pallas as pl
from jax.experimental.pallas import tpu as pltpu
from jax.sharding import PartitionSpec as P

AVG = 16
LANES = 128


def dft_table(slots):
    half = slots // 2
    q = np.arange(slots, dtype=np.int64).reshape(half, 2).T
    turns = (q[:, :, None] * np.arange(half, dtype=np.int64)) % slots
    angles = turns.astype(np.float64) * (-2.0 * math.pi / slots)
    table = np.concatenate([np.cos(angles), np.sin(angles)], axis=1).astype(np.float32)
    upper = table.astype(jnp.bfloat16)
    lower = (table - upper.astype(np.float32)).astype(jnp.bfloat16)
    return np.concatenate([upper, lower], axis=2)


def first_twist(slots, phases):
    half = slots // 2
    q = jnp.arange(slots, dtype=jnp.int32).reshape(half, 2).T
    q = jnp.broadcast_to(q[:, :, None], (2, half, LANES))
    angles = q.astype(jnp.float32) * jnp.float32(-2.0 * math.pi / (phases * slots))
    return jnp.stack([jnp.cos(angles), jnp.sin(angles)])


def channelise_kernel(spectra_count, a_ref, fir_ref, tab_ref, t1_ref, o_ref, xs, g, br, tw):
    phase = pl.program_id(0)
    groups, _, inputs, fr, slots = a_ref.shape
    frames = groups * fr
    taps = fir_ref.shape[1]
    half = slots // 2
    rows = inputs * frames

    @pl.when(phase == 0)
    def _():
        tw[0] = jnp.ones(tw.shape[1:], jnp.float32)
        tw[1] = jnp.zeros(tw.shape[1:], jnp.float32)
        xs[:, frames:, :] = jnp.zeros((inputs, xs.shape[1] - frames, slots), jnp.float32)

    for i in range(inputs):
        for grp in range(groups):
            xs[i, grp * fr : (grp + 1) * fr, :] = a_ref[grp, 0, i].astype(jnp.float32)

    keep = lax.broadcasted_iota(jnp.int32, (frames, LANES), 0) < spectra_count

    @pl.loop(0, inputs)
    def _(i):
        for chunk in range(half // LANES):

            def fir(at):
                total = None
                for k in range(taps):
                    term = fir_ref[0, k : k + 1, at : at + LANES] * xs[
                        i, taps - 1 - k : taps - 1 - k + frames, at : at + LANES
                    ]
                    total = term if total is None else total + term
                return jnp.where(keep, total, 0.0)

            at = chunk * LANES
            low, high = fir(at), fir(at + half)
            row = pl.multiple_of(i * frames, frames)
            for par, value in ((0, low + high), (1, low - high)):
                upper = value.astype(jnp.bfloat16)
                lower = (value - upper.astype(jnp.float32)).astype(jnp.bfloat16)
                g[par, pl.ds(row, frames), at : at + LANES] = upper
                g[par, pl.ds(row, frames), half + at : half + at + LANES] = upper
                g[par, pl.ds(row, frames), 2 * half + at : 2 * half + at + LANES] = lower

    step = 256
    dims = (((1,), (1,)), ((), ()))

    for par in range(2):

        @pl.loop(0, half // step)
        def _(block):
            def product(start):
                at = pl.multiple_of(start + block * step, step)
                first = tab_ref[par, pl.ds(at, step), :]
                return lax.dot_general(
                    first, g[par, :, : 2 * half], dims, preferred_element_type=jnp.float32
                ) + lax.dot_general(
                    first[:, :half], g[par, :, 2 * half :], dims, preferred_element_type=jnp.float32
                )

            real, imag = product(0), product(half)
            at = pl.multiple_of(block * step, step)
            cos = tw[0, par, pl.ds(at, step), :]
            sin = tw[1, par, pl.ds(at, step), :]
            for part in range(rows // LANES):
                re = real[:, part * LANES : (part + 1) * LANES]
                im = imag[:, part * LANES : (part + 1) * LANES]
                br[phase, 0, par, part, pl.ds(at, step), :] = (re * cos - im * sin).astype(jnp.bfloat16)
                br[phase, 1, par, part, pl.ds(at, step), :] = (re * sin + im * cos).astype(jnp.bfloat16)

    cos, sin = tw[0], tw[1]
    tw[0] = cos * t1_ref[0] - sin * t1_ref[1]
    tw[1] = cos * t1_ref[1] + sin * t1_ref[0]

    @pl.when(phase == pl.num_programs(0) - 1)
    def _():
        root = math.sqrt(0.5)
        tile = 16
        left = lax.broadcasted_iota(jnp.int32, (tile, LANES), 1) < frames

        def four(a, b, c, d):
            (ar, ai), (b_r, bi), (cr, ci), (dr, di) = a, b, c, d
            er, ei, fr_, fi = ar + cr, ai + ci, ar - cr, ai - ci
            gr, gi, hr, hi = b_r + dr, bi + di, b_r - dr, bi - di
            return ((er + gr, ei + gi), (fr_ + hi, fi - hr), (er - gr, ei - gi), (fr_ - hi, fi + hr))

        @pl.loop(0, half // tile)
        def _(block):
            at = pl.multiple_of(block * tile, tile)
            for part in range(rows // LANES):
                lines = []
                for par in range(2):
                    b = [
                        tuple(br[p, ri, par, part, pl.ds(at, tile), :].astype(jnp.float32) for ri in range(2))
                        for p in range(8)
                    ]
                    even = four(b[0], b[2], b[4], b[6])
                    odd = four(b[1], b[3], b[5], b[7])
                    (o1r, o1i), (o2r, o2i), (o3r, o3i) = odd[1:]
                    turned = (
                        odd[0],
                        ((o1r + o1i) * root, (o1i - o1r) * root),
                        (o2i, -o2r),
                        ((o3i - o3r) * root, (-o3r - o3i) * root),
                    )
                    lines.append([(e[0] + o[0], e[1] + o[1]) for e, o in zip(even, turned)])
                for c in range(4):
                    firsts, seconds = [], []
                    for par in range(2):
                        re, im = lines[par][c]
                        firsts.append(jnp.where(left, re, pltpu.roll(im, frames, 1)).reshape(2, 8, LANES))
                        seconds.append(jnp.where(left, pltpu.roll(re, frames, 1), im).reshape(2, 8, LANES))
                    for i, pair in ((2 * part, firsts), (2 * part + 1, seconds)):
                        both = jnp.concatenate(pair, axis=1)
                        o_ref[c, pl.ds(block * 2, 2), i] = both.astype(jnp.bfloat16)


def channelise(samples, fir_taps, spectra_count):
    groups, phases, inputs, fr, slots = samples.shape
    frames = groups * fr
    taps = fir_taps.shape[1]
    half = slots // 2
    rows = inputs * frames
    table = jnp.asarray(dft_table(slots))
    twist = first_twist(slots, phases)
    whole = pl.BlockSpec(memory_space=pltpu.VMEM)
    return pl.pallas_call(
        lambda *refs: channelise_kernel(spectra_count, *refs),
        grid=(phases,),
        out_shape=jax.ShapeDtypeStruct((4, slots // AVG, inputs, AVG, 2 * frames), jnp.bfloat16),
        in_specs=[
            pl.BlockSpec((groups, 1, inputs, fr, slots), lambda p: (0, p, 0, 0, 0)),
            pl.BlockSpec((1, taps, slots), lambda p: (p, 0, 0)),
            whole,
            whole,
        ],
        out_specs=whole,
        scratch_shapes=[
            pltpu.VMEM((inputs, frames + 8, slots), jnp.float32),
            pltpu.VMEM((2, rows, 3 * half), jnp.bfloat16),
            pltpu.VMEM((phases, 2, 2, rows // LANES, half, LANES), jnp.bfloat16),
            pltpu.VMEM((2, 2, half, LANES), jnp.float32),
        ],
        compiler_params=pltpu.CompilerParams(vmem_limit_bytes=60 << 20),
        cost_estimate=pl.CostEstimate(flops=20 * 10**9, bytes_accessed=20 << 20, transcendentals=0),
    )(samples, fir_taps, table, twist)


def correlate_kernel(scaling, r_ref, o_ref, wide, x, y):
    inputs, items, lanes = r_ref.shape
    step = 256
    dims = (((1,), (1,)), ((), ()))
    sub = 128

    @pl.loop(0, inputs // sub)
    def _(block):
        row = pl.multiple_of(block * sub, sub)
        wide[...] = r_ref[pl.ds(row, sub)].astype(jnp.float32).reshape(sub * items, lanes)
        left = lax.broadcasted_iota(jnp.int32, (sub, lanes), 1) < lanes // 2
        for item in range(items):
            value = wide[pl.ds(item, sub, stride=items), :]
            turned = pltpu.roll(value, lanes // 2, 1)
            at = item * lanes
            x[pl.ds(row, sub), at : at + lanes] = value.astype(jnp.bfloat16)
            y[pl.ds(row, sub), at : at + lanes] = jnp.where(left, turned, -turned).astype(jnp.bfloat16)

    @pl.loop(0, inputs // step)
    def _(block):
        row = pl.multiple_of(block * step, step)
        for part, source in ((0, x), (1, y)):
            for col in range(0, inputs, step):
                product = lax.dot_general(
                    source[pl.ds(row, step), :], x[col : col + step, :], dims, preferred_element_type=jnp.float32
                )
                o_ref[block, part, :, col : col + step] = (product * scaling).astype(jnp.bfloat16)


def correlate(gathered, scaling):
    inputs, items, lanes = gathered.shape
    whole = pl.BlockSpec(memory_space=pltpu.VMEM)
    return pl.pallas_call(
        lambda *refs: correlate_kernel(scaling, *refs),
        out_shape=jax.ShapeDtypeStruct((inputs // 256, 2, 256, inputs), jnp.bfloat16),
        in_specs=[whole],
        out_specs=whole,
        scratch_shapes=[
            pltpu.VMEM((128 * items, lanes), jnp.float32),
            pltpu.VMEM((inputs, items * lanes), jnp.bfloat16),
            pltpu.VMEM((inputs, items * lanes), jnp.bfloat16),
        ],
        compiler_params=pltpu.CompilerParams(vmem_limit_bytes=60 << 20),
        cost_estimate=pl.CostEstimate(flops=9 * 10**9, bytes_accessed=8 << 20, transcendentals=0),
    )(gathered)


def per_device(voltages, fir_taps):
    inputs_dev, _, fr, slots = voltages.shape
    phases, taps, _ = fir_taps.shape
    lane_count = lax.axis_size("chan")
    stations = lax.axis_size("stn")
    groups = lane_count // phases
    own = inputs_dev // lane_count
    frames = groups * fr
    spectra_count = frames - (taps - 1)
    dealt = lax.all_to_all(voltages[:, 0], "chan", 0, 0, tiled=True)
    samples = dealt.reshape(groups, phases, own, fr, slots)
    spectra = channelise(samples, fir_taps, spectra_count)
    spectra = spectra.reshape(stations * lane_count * own, AVG, 2 * frames)
    gathered = lax.all_to_all(spectra, ("stn", "chan"), 0, 0, tiled=True)
    scaling = 1.0 / (phases * slots * AVG * spectra_count)
    rows = correlate(gathered, scaling)
    mine = lax.all_to_all(rows, "stn", 0, 0, tiled=True)
    return mine.astype(jnp.float32)[:, None]


def solution(mesh):
    return jax.shard_map(
        per_device,
        mesh=mesh,
        in_specs=(P("stn", "chan", None, None), P()),
        out_specs=P(None, "chan", None, "stn", None),
        check_vma=False,
    )
```

```python
import math

import jax
import jax.numpy as jnp
import numpy as np
from jax import lax
from jax.experimental import pallas as pl
from jax.experimental.pallas import tpu as pltpu
from jax.sharding import PartitionSpec as P

AVG = 16
LANES = 128


def dft_table(slots, par):
    half = slots // 2
    q = 2 * np.arange(half, dtype=np.int64) + par
    turns = (q[:, None] * np.arange(half, dtype=np.int64)) % slots
    angles = turns.astype(np.float64) * (-2.0 * math.pi / slots)
    table = np.concatenate([np.cos(angles), np.sin(angles)]).astype(np.float32)
    upper = table.astype(jnp.bfloat16)
    lower = (table - upper.astype(np.float32)).astype(jnp.bfloat16)
    return np.concatenate([upper, lower], axis=1)


def first_twist(slots, phases, par):
    half = slots // 2
    q = 2 * jnp.arange(half, dtype=jnp.int32) + par
    q = jnp.broadcast_to(q[:, None], (half, LANES))
    angles = q.astype(jnp.float32) * jnp.float32(-2.0 * math.pi / (phases * slots))
    return jnp.stack([jnp.cos(angles), jnp.sin(angles)])


def transform(phase, g, tab_ref, t1_ref, br, tw):
    rows, half = g.shape[0], g.shape[1] // 2
    dims = (((1,), (1,)), ((), ()))

    @pl.when(phase == 0)
    def _():
        tw[0] = jnp.ones(tw.shape[1:], jnp.float32)
        tw[1] = jnp.zeros(tw.shape[1:], jnp.float32)

    def product(table, values):
        return lax.dot_general(table, values, dims, preferred_element_type=jnp.float32)

    upper, lower = g[:, :half], g[:, half:]
    both = (
        product(tab_ref[:, :half], upper)
        + product(tab_ref[:, half:], upper)
        + product(tab_ref[:, :half], lower)
    )
    cos, sin = tw[0], tw[1]
    for part in range(rows // LANES):
        re = both[:half, part * LANES : (part + 1) * LANES]
        im = both[half:, part * LANES : (part + 1) * LANES]
        br[phase, 0, part] = (re * cos - im * sin).astype(jnp.bfloat16)
        br[phase, 1, part] = (re * sin + im * cos).astype(jnp.bfloat16)
    tw[0] = cos * t1_ref[0] - sin * t1_ref[1]
    tw[1] = cos * t1_ref[1] + sin * t1_ref[0]


def bands(frames, br, o_ref, start, emit):
    phases, _, parts, half, _ = br.shape
    root = math.sqrt(0.5)
    tile = 16
    count = half // tile
    left = lax.broadcasted_iota(jnp.int32, (tile, LANES), 1) < frames

    def four(a, b, c, d):
        (ar, ai), (b_r, bi), (cr, ci), (dr, di) = a, b, c, d
        er, ei, fr_, fi = ar + cr, ai + ci, ar - cr, ai - ci
        gr, gi, hr, hi = b_r + dr, bi + di, b_r - dr, bi - di
        return ((er + gr, ei + gi), (fr_ + hi, fi - hr), (er - gr, ei - gi), (fr_ - hi, fi + hr))

    @pl.loop(0, count)
    def _(step):
        block = lax.rem(start + step, count)
        at = pl.multiple_of(block * tile, tile)
        for part in range(parts):
            b = [
                tuple(br[p, ri, part, pl.ds(at, tile), :].astype(jnp.float32) for ri in range(2))
                for p in range(8)
            ]
            even = four(b[0], b[2], b[4], b[6])
            odd = four(b[1], b[3], b[5], b[7])
            (o1r, o1i), (o2r, o2i), (o3r, o3i) = odd[1:]
            turned = (
                odd[0],
                ((o1r + o1i) * root, (o1i - o1r) * root),
                (o2i, -o2r),
                ((o3i - o3r) * root, (-o3r - o3i) * root),
            )
            for c in range(4):
                re = even[c][0] + turned[c][0]
                im = even[c][1] + turned[c][1]
                first = jnp.where(left, re, pltpu.roll(im, frames, 1)).reshape(2, 8, LANES)
                second = jnp.where(left, pltpu.roll(re, frames, 1), im).reshape(2, 8, LANES)
                both = jnp.concatenate([first, second], axis=1)
                o_ref[c, pl.ds(block * 2, 2), part] = both.astype(jnp.bfloat16)

        @pl.when(step > 0)
        def _():
            emit(lax.rem(start + step + count - 1, count))

    emit(lax.rem(start + count - 1, count))


def channelise_kernel(
    spectra_count, a_ref, fir_ref, tab_ref, t1_ref, r0_ref, r1_ref, xs, g, later, br, tw, out, send_sem, recv_sem
):
    phase = pl.program_id(0)
    groups, _, inputs, fr, slots = a_ref.shape
    frames = groups * fr
    taps = fir_ref.shape[1]
    half = slots // 2
    stations, spans = out.shape[1], out.shape[2]
    my_stn, my_chan = lax.axis_index("stn"), lax.axis_index("chan")
    me = my_stn * spans + my_chan

    @pl.when(phase == 0)
    def _():
        xs[:, :, frames:, :] = jnp.zeros((inputs, slots // LANES, xs.shape[2] - frames, LANES), jnp.float32)

    for i in range(inputs):
        for grp in range(groups):
            line = a_ref[grp, 0, i].astype(jnp.float32)
            for col in range(slots // LANES):
                xs[i, col, grp * fr : (grp + 1) * fr, :] = line[:, col * LANES : (col + 1) * LANES]

    keep = lax.broadcasted_iota(jnp.int32, (frames, LANES), 0) < spectra_count

    @pl.loop(0, inputs)
    def _(i):
        for chunk in range(half // LANES):

            def fir(at):
                total = None
                for k in range(taps):
                    term = fir_ref[0, k : k + 1, at : at + LANES] * xs[
                        i, at // LANES, taps - 1 - k : taps - 1 - k + frames, :
                    ]
                    total = term if total is None else total + term
                return jnp.where(keep, total, 0.0)

            at = chunk * LANES
            low, high = fir(at), fir(at + half)
            row = pl.multiple_of(i * frames, frames)

            def keep_split(value, store):
                upper = value.astype(jnp.bfloat16)
                store(at, upper)
                store(half + at, (value - upper.astype(jnp.float32)).astype(jnp.bfloat16))

            def now(lane, value):
                g[pl.ds(row, frames), lane : lane + LANES] = value

            def after(lane, value):
                later[phase, pl.ds(row, frames), lane : lane + LANES] = value

            keep_split(low + high, now)
            keep_split(low - high, after)

    transform(phase, g, tab_ref.at[0], t1_ref.at[0], br, tw)

    def emit(par, target):
        def blocks(block):
            for turn in range(2):
                u = 2 * block + lax.rem(my_chan + turn, 2)
                for shift in range(stations):
                    c = lax.rem(my_stn + shift, stations)
                    source, landing = out.at[par, c, u], target.at[me]
                    mine = jnp.logical_and(shift == 0, u == my_chan)

                    @pl.when(mine)
                    def _():
                        pltpu.make_async_copy(source, landing, recv_sem.at[par]).start()

                    @pl.when(jnp.logical_not(mine))
                    def _():
                        pltpu.make_async_remote_copy(
                            src_ref=source,
                            dst_ref=landing,
                            send_sem=send_sem.at[par],
                            recv_sem=recv_sem.at[par],
                            device_id=(c, u),
                            device_id_type=pl.DeviceIdType.MESH,
                        ).start()

        return blocks

    @pl.when(phase == pl.num_programs(0) - 1)
    def _():
        start = my_chan // 2
        bands(frames, br, out.at[0], start, emit(0, r0_ref))

        @pl.loop(0, later.shape[0])
        def _(p):
            transform(p, later.at[p], tab_ref.at[1], t1_ref.at[1], br, tw)

        bands(frames, br, out.at[1], start, emit(1, r1_ref))
        for par, target in ((0, r0_ref), (1, r1_ref)):
            pltpu.make_async_copy(target, target, recv_sem.at[par]).wait()
            others = target.at[pl.ds(0, stations * spans - 1)]
            pltpu.make_async_copy(others, others, send_sem.at[par]).wait()


def channelise(samples, fir_taps, spectra_count, stations):
    groups, phases, inputs, fr, slots = samples.shape
    frames = groups * fr
    taps = fir_taps.shape[1]
    half = slots // 2
    rows = inputs * frames
    parts = rows // LANES
    spans = slots // AVG
    whole = pl.BlockSpec(memory_space=pltpu.VMEM)
    landing = jax.ShapeDtypeStruct((stations * spans, parts, AVG, LANES), jnp.bfloat16)
    table = np.stack([dft_table(slots, par) for par in range(2)])
    twist = jnp.stack([first_twist(slots, phases, par) for par in range(2)])
    return pl.pallas_call(
        lambda *refs: channelise_kernel(spectra_count, *refs),
        grid=(phases,),
        out_shape=(landing, landing),
        in_specs=[
            pl.BlockSpec((groups, 1, inputs, fr, slots), lambda p: (0, p, 0, 0, 0)),
            pl.BlockSpec((1, taps, slots), lambda p: (p, 0, 0)),
            whole,
            whole,
        ],
        out_specs=[pl.BlockSpec(memory_space=pl.ANY)] * 2,
        scratch_shapes=[
            pltpu.VMEM((inputs, slots // LANES, frames + 8, LANES), jnp.float32),
            pltpu.VMEM((rows, slots), jnp.bfloat16),
            pltpu.VMEM((phases, rows, slots), jnp.bfloat16),
            pltpu.VMEM((phases, 2, parts, half, LANES), jnp.bfloat16),
            pltpu.VMEM((2, half, LANES), jnp.float32),
            pltpu.VMEM((2, stations, spans, parts, AVG, LANES), jnp.bfloat16),
            pltpu.SemaphoreType.DMA((2,)),
            pltpu.SemaphoreType.DMA((2,)),
        ],
        compiler_params=pltpu.CompilerParams(vmem_limit_bytes=60 << 20, has_side_effects=True),
        cost_estimate=pl.CostEstimate(flops=20 * 10**9, bytes_accessed=20 << 20, transcendentals=0),
    )(samples, fir_taps, jnp.asarray(table), twist)


def correlate_kernel(scaling, r0_ref, r1_ref, o_ref, wide, x, y):
    inputs, lanes = x.shape[0], LANES
    items = x.shape[1] // lanes // 2
    sub = wide.shape[0] // items
    tiles = sub * items // AVG
    dims = (((1,), (1,)), ((), ()))

    @pl.when(pl.program_id(0) == 0)
    def _():
        for par, r_ref in ((0, r0_ref), (1, r1_ref)):

            @pl.loop(0, inputs // sub)
            def _(block):
                row = pl.multiple_of(block * sub, sub)
                at = pl.multiple_of(block * tiles, tiles)
                wide[...] = r_ref[pl.ds(at, tiles)].astype(jnp.float32).reshape(sub * items, lanes)
                left = lax.broadcasted_iota(jnp.int32, (sub, lanes), 1) < lanes // 2
                for item in range(items):
                    value = wide[pl.ds(item, sub, stride=items), :]
                    turned = pltpu.roll(value, lanes // 2, 1)
                    lane = (par * items + item) * lanes
                    x[pl.ds(row, sub), lane : lane + lanes] = value.astype(jnp.bfloat16)
                    y[pl.ds(row, sub), lane : lane + lanes] = jnp.where(left, turned, -turned).astype(jnp.bfloat16)

    rows = o_ref.shape[2]
    at = pl.multiple_of(pl.program_id(0) * rows, rows)
    for part, source in ((0, x), (1, y)):
        product = lax.dot_general(source[pl.ds(at, rows), :], x[...], dims, preferred_element_type=jnp.float32)
        o_ref[0, part] = (product * scaling).astype(o_ref.dtype)


def correlate(first, second, scaling, inputs):
    items = first.shape[0] * AVG // inputs
    rows = 256
    whole = pl.BlockSpec(memory_space=pltpu.VMEM)
    return pl.pallas_call(
        lambda *refs: correlate_kernel(scaling, *refs),
        grid=(inputs // rows,),
        out_shape=jax.ShapeDtypeStruct((inputs // rows, 2, rows, inputs), jnp.bfloat16),
        in_specs=[whole, whole],
        out_specs=pl.BlockSpec((1, 2, rows, inputs), lambda j: (j, 0, 0, 0)),
        scratch_shapes=[
            pltpu.VMEM((128 * items, LANES), jnp.float32),
            pltpu.VMEM((inputs, 2 * items * LANES), jnp.bfloat16),
            pltpu.VMEM((inputs, 2 * items * LANES), jnp.bfloat16),
        ],
        compiler_params=pltpu.CompilerParams(vmem_limit_bytes=60 << 20),
        cost_estimate=pl.CostEstimate(flops=9 * 10**9, bytes_accessed=12 << 20, transcendentals=0),
    )(first, second)


def per_device(voltages, fir_taps):
    inputs_dev, _, fr, slots = voltages.shape
    phases, taps, _ = fir_taps.shape
    lane_count = lax.axis_size("chan")
    stations = lax.axis_size("stn")
    groups = lane_count // phases
    own = inputs_dev // lane_count
    frames = groups * fr
    spectra_count = frames - (taps - 1)
    dealt = lax.all_to_all(voltages[:, 0], "chan", 0, 0, tiled=True)
    samples = dealt.reshape(groups, phases, own, fr, slots)
    first, second = channelise(samples, fir_taps, spectra_count, stations)
    inputs = inputs_dev * stations
    scaling = 1.0 / (phases * slots * AVG * spectra_count)
    rows = correlate(first.reshape(-1, AVG, LANES), second.reshape(-1, AVG, LANES), scaling, inputs)
    mine = lax.all_to_all(rows, "stn", 0, 0, tiled=True)
    return mine.astype(jnp.float32)[:, None]


def solution(mesh):
    return jax.shard_map(
        per_device,
        mesh=mesh,
        in_specs=(P("stn", "chan", None, None), P()),
        out_specs=P(None, "chan", None, "stn", None),
        check_vma=False,
    )
```

```python
import math

import jax
import jax.numpy as jnp
import numpy as np
from jax import lax
from jax.experimental import pallas as pl
from jax.experimental.pallas import tpu as pltpu
from jax.sharding import PartitionSpec as P

AVG = 16
LANES = 128


def dft_table(slots, par):
    half = slots // 2
    q = 2 * np.arange(half, dtype=np.int64) + par
    turns = (q[:, None] * np.arange(half, dtype=np.int64)) % slots
    angles = turns.astype(np.float64) * (-2.0 * math.pi / slots)
    table = np.concatenate([np.cos(angles), np.sin(angles)]).astype(np.float32)
    upper = table.astype(jnp.bfloat16)
    lower = (table - upper.astype(np.float32)).astype(jnp.bfloat16)
    return np.concatenate([upper, lower], axis=1)


def first_twist(slots, phases, par):
    half = slots // 2
    q = 2 * jnp.arange(half, dtype=jnp.int32) + par
    q = jnp.broadcast_to(q[:, None], (half, LANES))
    angles = q.astype(jnp.float32) * jnp.float32(-2.0 * math.pi / (phases * slots))
    return jnp.stack([jnp.cos(angles), jnp.sin(angles)])


def transform(phase, g, tab_ref, t1_ref, br, tw):
    rows, half = g.shape[0], g.shape[1] // 2
    dims = (((1,), (1,)), ((), ()))

    @pl.when(phase == 0)
    def _():
        tw[0] = jnp.ones(tw.shape[1:], jnp.float32)
        tw[1] = jnp.zeros(tw.shape[1:], jnp.float32)

    def product(table, values):
        return lax.dot_general(table, values, dims, preferred_element_type=jnp.float32)

    upper, lower = g[:, :half], g[:, half:]
    both = (
        product(tab_ref[:, :half], upper)
        + product(tab_ref[:, half:], upper)
        + product(tab_ref[:, :half], lower)
    )
    cos, sin = tw[0], tw[1]
    for part in range(rows // LANES):
        re = both[:half, part * LANES : (part + 1) * LANES]
        im = both[half:, part * LANES : (part + 1) * LANES]
        br[phase, 0, part] = (re * cos - im * sin).astype(jnp.bfloat16)
        br[phase, 1, part] = (re * sin + im * cos).astype(jnp.bfloat16)
    tw[0] = cos * t1_ref[0] - sin * t1_ref[1]
    tw[1] = cos * t1_ref[1] + sin * t1_ref[0]


def bands(frames, br, o_ref, start, emit):
    phases, _, parts, half, _ = br.shape
    root = math.sqrt(0.5)
    tile = 16
    count = half // tile
    left = lax.broadcasted_iota(jnp.int32, (tile, LANES), 1) < frames

    def four(a, b, c, d):
        (ar, ai), (b_r, bi), (cr, ci), (dr, di) = a, b, c, d
        er, ei, fr_, fi = ar + cr, ai + ci, ar - cr, ai - ci
        gr, gi, hr, hi = b_r + dr, bi + di, b_r - dr, bi - di
        return ((er + gr, ei + gi), (fr_ + hi, fi - hr), (er - gr, ei - gi), (fr_ - hi, fi + hr))

    @pl.loop(0, count)
    def _(step):
        block = lax.rem(start + step, count)
        at = pl.multiple_of(block * tile, tile)
        for part in range(parts):
            b = [
                tuple(br[p, ri, part, pl.ds(at, tile), :].astype(jnp.float32) for ri in range(2))
                for p in range(8)
            ]
            even = four(b[0], b[2], b[4], b[6])
            odd = four(b[1], b[3], b[5], b[7])
            (o1r, o1i), (o2r, o2i), (o3r, o3i) = odd[1:]
            turned = (
                odd[0],
                ((o1r + o1i) * root, (o1i - o1r) * root),
                (o2i, -o2r),
                ((o3i - o3r) * root, (-o3r - o3i) * root),
            )
            for c in range(4):
                re = even[c][0] + turned[c][0]
                im = even[c][1] + turned[c][1]
                first = jnp.where(left, re, pltpu.roll(im, frames, 1)).reshape(2, 8, LANES)
                second = jnp.where(left, pltpu.roll(re, frames, 1), im).reshape(2, 8, LANES)
                both = jnp.concatenate([first, second], axis=1)
                o_ref[c, pl.ds(block * 2, 2), part] = both.astype(jnp.bfloat16)

        @pl.when(step > 0)
        def _():
            emit(lax.rem(start + step + count - 1, count))

    emit(lax.rem(start + count - 1, count))


def spread(r_ref, wide, x, y):
    inputs, lanes = x.shape[0], LANES
    items = x.shape[1] // lanes
    sub = wide.shape[0] // items
    tiles = sub * items // AVG

    @pl.loop(0, inputs // sub)
    def _(block):
        row = pl.multiple_of(block * sub, sub)
        at = pl.multiple_of(block * tiles, tiles)
        wide[...] = r_ref[pl.ds(at, tiles)].astype(jnp.float32).reshape(sub * items, lanes)
        left = lax.broadcasted_iota(jnp.int32, (sub, lanes), 1) < lanes // 2
        for item in range(items):
            value = wide[pl.ds(item, sub, stride=items), :]
            turned = pltpu.roll(value, lanes // 2, 1)
            lane = item * lanes
            x[pl.ds(row, sub), lane : lane + lanes] = value.astype(jnp.bfloat16)
            y[pl.ds(row, sub), lane : lane + lanes] = jnp.where(left, turned, -turned).astype(jnp.bfloat16)


def channelise_kernel(
    spectra_count,
    scaling,
    a_ref,
    fir_ref,
    tab_ref,
    t1_ref,
    v_ref,
    xs,
    g,
    later,
    br,
    tw,
    out,
    landed,
    wide,
    x,
    y,
    partial,
    rows_out,
    send_sem,
    recv_sem,
    row_send,
    row_recv,
):
    phase = pl.program_id(0)
    groups, _, inputs, fr, slots = a_ref.shape
    frames = groups * fr
    taps = fir_ref.shape[1]
    half = slots // 2
    stations, spans = out.shape[1], out.shape[2]
    my_stn, my_chan = lax.axis_index("stn"), lax.axis_index("chan")
    me = my_stn * spans + my_chan

    @pl.when(phase == 0)
    def _():
        xs[:, :, frames:, :] = jnp.zeros((inputs, slots // LANES, xs.shape[2] - frames, LANES), jnp.float32)

    for i in range(inputs):
        for grp in range(groups):
            line = a_ref[grp, 0, i].astype(jnp.float32)
            for col in range(slots // LANES):
                xs[i, col, grp * fr : (grp + 1) * fr, :] = line[:, col * LANES : (col + 1) * LANES]

    keep = lax.broadcasted_iota(jnp.int32, (frames, LANES), 0) < spectra_count

    @pl.loop(0, inputs)
    def _(i):
        for chunk in range(half // LANES):

            def fir(at):
                total = None
                for k in range(taps):
                    term = fir_ref[0, k : k + 1, at : at + LANES] * xs[
                        i, at // LANES, taps - 1 - k : taps - 1 - k + frames, :
                    ]
                    total = term if total is None else total + term
                return jnp.where(keep, total, 0.0)

            at = chunk * LANES
            low, high = fir(at), fir(at + half)
            row = pl.multiple_of(i * frames, frames)

            def keep_split(value, store):
                upper = value.astype(jnp.bfloat16)
                store(at, upper)
                store(half + at, (value - upper.astype(jnp.float32)).astype(jnp.bfloat16))

            def now(lane, value):
                g[pl.ds(row, frames), lane : lane + LANES] = value

            def after(lane, value):
                later[phase, pl.ds(row, frames), lane : lane + LANES] = value

            keep_split(low + high, now)
            keep_split(low - high, after)

    transform(phase, g, tab_ref.at[0], t1_ref.at[0], br, tw)

    slots_each = landed.shape[1] // (stations * spans)

    def emit(par):
        def blocks(block):
            for turn in range(2):
                u = 2 * block + lax.rem(my_chan + turn, 2)
                for shift in range(stations):
                    c = lax.rem(my_stn + shift, stations)
                    source = out.at[par, c, u]
                    landing = landed.at[par, pl.ds(me * slots_each, slots_each)]
                    mine = jnp.logical_and(shift == 0, u == my_chan)

                    @pl.when(mine)
                    def _():
                        pltpu.make_async_copy(source, landing, recv_sem.at[par]).start()

                    @pl.when(jnp.logical_not(mine))
                    def _():
                        pltpu.make_async_remote_copy(
                            src_ref=source,
                            dst_ref=landing,
                            send_sem=send_sem.at[par],
                            recv_sem=recv_sem.at[par],
                            device_id=(c, u),
                            device_id_type=pl.DeviceIdType.MESH,
                        ).start()

        return blocks

    @pl.when(phase == pl.num_programs(0) - 1)
    def _():
        start = my_chan // 2
        bands(frames, br, out.at[0], start, emit(0))

        @pl.loop(0, later.shape[0])
        def _(p):
            transform(p, later.at[p], tab_ref.at[1], t1_ref.at[1], br, tw)

        bands(frames, br, out.at[1], start, emit(1))

        dims = (((1,), (1,)), ((), ()))
        height = rows_out.shape[2]

        def product(j, part):
            source = (x, y)[part]
            at = pl.multiple_of(j * height, height)
            return lax.dot_general(source[pl.ds(at, height), :], x[...], dims, preferred_element_type=jnp.float32)

        def arrived(par):
            pltpu.make_async_copy(landed.at[par], landed.at[par], recv_sem.at[par]).wait()

        arrived(0)
        spread(landed.at[0], wide, x, y)

        @pl.loop(0, stations)
        def _(j):
            for part in range(2):
                partial[j, part] = product(j, part)

        arrived(1)
        spread(landed.at[1], wide, x, y)

        def owner(turn):
            return lax.rem(my_stn + jnp.where(turn < 2, 2 + turn, 3 - turn), stations)

        def send(j, part):
            source, landing = rows_out.at[j, part], v_ref.at[my_stn, part]

            @pl.when(j == my_stn)
            def _():
                pltpu.make_async_copy(source, landing, row_recv).start()

            @pl.when(j != my_stn)
            def _():
                pltpu.make_async_remote_copy(
                    src_ref=source,
                    dst_ref=landing,
                    send_sem=row_send,
                    recv_sem=row_recv,
                    device_id=(j, my_chan),
                    device_id_type=pl.DeviceIdType.MESH,
                ).start()

        def finish(j, part):
            total = (partial[j, part] + product(j, part)) * scaling
            rows_out[j, part] = total.astype(rows_out.dtype)

        @pl.loop(0, stations)
        def _(turn):
            j = owner(turn)
            finish(j, 0)

            @pl.when(turn > 0)
            def _():
                send(owner(turn - 1), 1)

            finish(j, 1)
            send(j, 0)

        send(owner(stations - 1), 1)
        for par in range(2):
            others = landed.at[par, pl.ds(0, landed.shape[1] - slots_each)]
            pltpu.make_async_copy(others, others, send_sem.at[par]).wait()
        pltpu.make_async_copy(v_ref, v_ref, row_recv).wait()
        others = v_ref.at[pl.ds(0, stations - 1)]
        pltpu.make_async_copy(others, others, row_send).wait()


def correlate(samples, fir_taps, spectra_count, scaling, stations, rows_dev):
    groups, phases, inputs, fr, slots = samples.shape
    frames = groups * fr
    taps = fir_taps.shape[1]
    half = slots // 2
    rows = inputs * frames
    parts = rows // LANES
    spans = slots // AVG
    whole = pl.BlockSpec(memory_space=pltpu.VMEM)
    whole_inputs = stations * rows_dev
    depth = AVG // 2 * LANES
    table = np.stack([dft_table(slots, par) for par in range(2)])
    twist = jnp.stack([first_twist(slots, phases, par) for par in range(2)])
    return pl.pallas_call(
        lambda *refs: channelise_kernel(spectra_count, scaling, *refs),
        grid=(phases,),
        out_shape=jax.ShapeDtypeStruct((stations, 2, rows_dev, whole_inputs), jnp.bfloat16),
        in_specs=[
            pl.BlockSpec((groups, 1, inputs, fr, slots), lambda p: (0, p, 0, 0, 0)),
            pl.BlockSpec((1, taps, slots), lambda p: (p, 0, 0)),
            whole,
            whole,
        ],
        out_specs=pl.BlockSpec(memory_space=pl.ANY),
        scratch_shapes=[
            pltpu.VMEM((inputs, slots // LANES, frames + 8, LANES), jnp.float32),
            pltpu.VMEM((rows, slots), jnp.bfloat16),
            pltpu.VMEM((phases, rows, slots), jnp.bfloat16),
            pltpu.VMEM((phases, 2, parts, half, LANES), jnp.bfloat16),
            pltpu.VMEM((2, half, LANES), jnp.float32),
            pltpu.VMEM((2, stations, spans, parts, AVG, LANES), jnp.bfloat16),
            pltpu.VMEM((2, stations * spans * parts, AVG, LANES), jnp.bfloat16),
            pltpu.VMEM((LANES * AVG // 2, LANES), jnp.float32),
            pltpu.VMEM((whole_inputs, depth), jnp.bfloat16),
            pltpu.VMEM((whole_inputs, depth), jnp.bfloat16),
            pltpu.VMEM((stations, 2, rows_dev, whole_inputs), jnp.float32),
            pltpu.VMEM((stations, 2, rows_dev, whole_inputs), jnp.bfloat16),
            pltpu.SemaphoreType.DMA((2,)),
            pltpu.SemaphoreType.DMA((2,)),
            pltpu.SemaphoreType.DMA,
            pltpu.SemaphoreType.DMA,
        ],
        compiler_params=pltpu.CompilerParams(vmem_limit_bytes=60 << 20, has_side_effects=True),
        cost_estimate=pl.CostEstimate(flops=30 * 10**9, bytes_accessed=20 << 20, transcendentals=0),
    )(samples, fir_taps, jnp.asarray(table), twist)


def per_device(voltages, fir_taps):
    inputs_dev, _, fr, slots = voltages.shape
    phases, taps, _ = fir_taps.shape
    lane_count = lax.axis_size("chan")
    stations = lax.axis_size("stn")
    groups = lane_count // phases
    own = inputs_dev // lane_count
    frames = groups * fr
    spectra_count = frames - (taps - 1)
    dealt = lax.all_to_all(voltages[:, 0], "chan", 0, 0, tiled=True)
    samples = dealt.reshape(groups, phases, own, fr, slots)
    scaling = 1.0 / (phases * slots * AVG * spectra_count)
    mine = correlate(samples, fir_taps, spectra_count, scaling, stations, inputs_dev)
    return mine.astype(jnp.float32)[:, None]


def solution(mesh):
    return jax.shard_map(
        per_device,
        mesh=mesh,
        in_specs=(P("stn", "chan", None, None), P()),
        out_specs=P(None, "chan", None, "stn", None),
        check_vma=False,
    )
```

```python
import math

import jax
import jax.numpy as jnp
import numpy as np
from jax import lax
from jax.experimental import pallas as pl
from jax.experimental.pallas import tpu as pltpu
from jax.sharding import PartitionSpec as P

AVG = 16
LANES = 128


def dft_table(slots, par):
    half = slots // 2
    q = 2 * np.arange(half, dtype=np.int64) + par
    turns = (q[:, None] * np.arange(half, dtype=np.int64)) % slots
    angles = turns.astype(np.float64) * (-2.0 * math.pi / slots)
    parts = np.stack([np.cos(angles), np.sin(angles)]).reshape(2, 2, half // 2, half)
    table = parts.transpose(1, 0, 2, 3).reshape(slots, half).astype(np.float32)
    upper = table.astype(jnp.bfloat16)
    lower = (table - upper.astype(np.float32)).astype(jnp.bfloat16)
    return np.concatenate([upper, lower], axis=1)


def first_twist(slots, phases, par):
    half = slots // 2
    q = 2 * jnp.arange(half, dtype=jnp.int32) + par
    q = jnp.broadcast_to(q[:, None], (half, LANES))
    angles = q.astype(jnp.float32) * jnp.float32(-2.0 * math.pi / (phases * slots))
    return jnp.stack([jnp.cos(angles), jnp.sin(angles)])


def transform(phase, at, g, tab_ref, t1_ref, br, tw):
    rows, half = g.shape[0], g.shape[1] // 2
    size = half // 2
    dims = (((1,), (1,)), ((), ()))

    @pl.when(phase == 0)
    def _():
        tw[0] = jnp.ones(tw.shape[1:], jnp.float32)
        tw[1] = jnp.zeros(tw.shape[1:], jnp.float32)

    def product(table, values):
        return lax.dot_general(table, values, dims, preferred_element_type=jnp.float32)

    upper, lower = g[:, :half], g[:, half:]
    both = (
        product(tab_ref[:, :half], upper)
        + product(tab_ref[:, half:], upper)
        + product(tab_ref[:, :half], lower)
    )
    cos, sin = tw[0], tw[1]
    for part in range(rows // LANES):
        re = both[:size, part * LANES : (part + 1) * LANES]
        im = both[size:, part * LANES : (part + 1) * LANES]
        br[phase, 0, part] = (re * cos - im * sin).astype(jnp.bfloat16)
        br[phase, 1, part] = (re * sin + im * cos).astype(jnp.bfloat16)
    first, second = t1_ref[0, pl.ds(at, size), :], t1_ref[1, pl.ds(at, size), :]
    tw[0] = cos * first - sin * second
    tw[1] = cos * second + sin * first


def bands(frames, br, o_ref, base, start, emit):
    phases, _, parts, half, _ = br.shape
    root = math.sqrt(0.5)
    tile = 16
    count = half // tile
    left = lax.broadcasted_iota(jnp.int32, (tile, LANES), 1) < frames

    def four(a, b, c, d):
        (ar, ai), (b_r, bi), (cr, ci), (dr, di) = a, b, c, d
        er, ei, fr_, fi = ar + cr, ai + ci, ar - cr, ai - ci
        gr, gi, hr, hi = b_r + dr, bi + di, b_r - dr, bi - di
        return ((er + gr, ei + gi), (fr_ + hi, fi - hr), (er - gr, ei - gi), (fr_ - hi, fi + hr))

    @pl.loop(0, count)
    def _(step):
        block = lax.rem(start + step, count)
        at = pl.multiple_of(block * tile, tile)
        for part in range(parts):
            b = [
                tuple(br[p, ri, part, pl.ds(at, tile), :].astype(jnp.float32) for ri in range(2))
                for p in range(8)
            ]
            even = four(b[0], b[2], b[4], b[6])
            odd = four(b[1], b[3], b[5], b[7])
            (o1r, o1i), (o2r, o2i), (o3r, o3i) = odd[1:]
            turned = (
                odd[0],
                ((o1r + o1i) * root, (o1i - o1r) * root),
                (o2i, -o2r),
                ((o3i - o3r) * root, (-o3r - o3i) * root),
            )
            for c in range(4):
                re = even[c][0] + turned[c][0]
                im = even[c][1] + turned[c][1]
                first = jnp.where(left, re, pltpu.roll(im, frames, 1)).reshape(2, 8, LANES)
                second = jnp.where(left, pltpu.roll(re, frames, 1), im).reshape(2, 8, LANES)
                both = jnp.concatenate([first, second], axis=1)
                o_ref[c, pl.ds((base + block) * 2, 2), part] = both.astype(jnp.bfloat16)

        @pl.when(step > 0)
        def _():
            emit(base + lax.rem(start + step + count - 1, count))

    emit(base + lax.rem(start + count - 1, count))


def spread(r_ref, wide, x, y):
    inputs, lanes = x.shape[0], LANES
    items = x.shape[1] // lanes
    sub = wide.shape[0] // items
    tiles = sub * items // AVG

    @pl.loop(0, inputs // sub)
    def _(block):
        row = pl.multiple_of(block * sub, sub)
        at = pl.multiple_of(block * tiles, tiles)
        wide[...] = r_ref[pl.ds(at, tiles)].astype(jnp.float32).reshape(sub * items, lanes)
        left = lax.broadcasted_iota(jnp.int32, (sub, lanes), 1) < lanes // 2
        for item in range(items):
            value = wide[pl.ds(item, sub, stride=items), :]
            turned = pltpu.roll(value, lanes // 2, 1)
            lane = item * lanes
            x[pl.ds(row, sub), lane : lane + lanes] = value.astype(jnp.bfloat16)
            y[pl.ds(row, sub), lane : lane + lanes] = jnp.where(left, turned, -turned).astype(jnp.bfloat16)


def channelise_kernel(
    spectra_count,
    scaling,
    volt_ref,
    fir_ref,
    tab_ref,
    t1_ref,
    v_ref,
    inbox,
    xs,
    g,
    br,
    tw,
    out,
    landed,
    wide,
    x,
    y,
    partial,
    rows_out,
    in_send,
    in_recv,
    send_sem,
    recv_sem,
    row_send,
    row_recv,
):
    inputs, lane_count, fr, slots = inbox.shape
    phases, taps, _ = fir_ref.shape
    groups = lane_count // phases
    frames = groups * fr
    half = slots // 2
    stations, spans = out.shape[1], out.shape[2]
    my_stn, my_chan = lax.axis_index("stn"), lax.axis_index("chan")
    me = my_stn * spans + my_chan

    for i in range(inputs):

        @pl.loop(0, lane_count)
        def _(shift):
            lane = lax.rem(my_chan + shift, lane_count)
            source, landing = volt_ref.at[lane * inputs + i], inbox.at[i, my_chan]

            @pl.when(shift == 0)
            def _():
                pltpu.make_async_copy(source, landing, in_recv.at[i]).start()

            @pl.when(shift != 0)
            def _():
                pltpu.make_async_remote_copy(
                    src_ref=source,
                    dst_ref=landing,
                    send_sem=in_send.at[i],
                    recv_sem=in_recv.at[i],
                    device_id=(my_stn, lane),
                    device_id_type=pl.DeviceIdType.MESH,
                ).start()

    xs[:, frames:, :] = jnp.zeros((slots // LANES, xs.shape[1] - frames, LANES), jnp.float32)
    keep = lax.broadcasted_iota(jnp.int32, (frames, LANES), 0) < spectra_count

    @pl.loop(0, inputs)
    def _(i):
        pltpu.make_async_copy(inbox.at[i], inbox.at[i], in_recv.at[i]).wait()
        row = pl.multiple_of(i * frames, frames)

        @pl.loop(0, phases)
        def _(phase):
            for grp in range(groups):
                line = inbox[i, grp * phases + phase].astype(jnp.float32)
                for col in range(slots // LANES):
                    xs[col, grp * fr : (grp + 1) * fr, :] = line[:, col * LANES : (col + 1) * LANES]

            for chunk in range(half // LANES):

                def fir(at):
                    total = None
                    for k in range(taps):
                        term = fir_ref[phase, k : k + 1, at : at + LANES] * xs[
                            at // LANES, taps - 1 - k : taps - 1 - k + frames, :
                        ]
                        total = term if total is None else total + term
                    return jnp.where(keep, total, 0.0)

                at = chunk * LANES
                low, high = fir(at), fir(at + half)
                for par, value in ((0, low + high), (1, low - high)):
                    upper = value.astype(jnp.bfloat16)
                    lower = (value - upper.astype(jnp.float32)).astype(jnp.bfloat16)
                    g[par, phase, pl.ds(row, frames), at : at + LANES] = upper
                    g[par, phase, pl.ds(row, frames), half + at : half + at + LANES] = lower

    slots_each = landed.shape[1] // (stations * spans)

    def emit(par):
        def blocks(block):
            for turn in range(2):
                u = 2 * block + lax.rem(my_chan + turn, 2)
                for shift in range(stations):
                    c = lax.rem(my_stn + shift, stations)
                    source = out.at[par, c, u]
                    landing = landed.at[par, pl.ds(me * slots_each, slots_each)]
                    mine = jnp.logical_and(shift == 0, u == my_chan)

                    @pl.when(mine)
                    def _():
                        pltpu.make_async_copy(source, landing, recv_sem.at[par]).start()

                    @pl.when(jnp.logical_not(mine))
                    def _():
                        pltpu.make_async_remote_copy(
                            src_ref=source,
                            dst_ref=landing,
                            send_sem=send_sem.at[par],
                            recv_sem=recv_sem.at[par],
                            device_id=(c, u),
                            device_id_type=pl.DeviceIdType.MESH,
                        ).start()

        return blocks

    size = half // 2
    count = size // AVG
    own_half = my_chan // (spans // 2)
    for par in range(2):
        for turn in range(2):
            which = lax.rem(own_half + turn, 2)
            at = pl.multiple_of(which * size, size)
            table = tab_ref.at[par, pl.ds(pl.multiple_of(which * half, half), half)]

            @pl.loop(0, phases)
            def _(phase):
                transform(phase, at, g.at[par, phase], table, t1_ref.at[par], br, tw)

            bands(frames, br, out.at[par], which * count, lax.rem(my_chan // 2, count), emit(par))

    dims = (((1,), (1,)), ((), ()))
    height = rows_out.shape[2]

    def product(j, part):
        source = (x, y)[part]
        at = pl.multiple_of(j * height, height)
        return lax.dot_general(source[pl.ds(at, height), :], x[...], dims, preferred_element_type=jnp.float32)

    def arrived(par):
        pltpu.make_async_copy(landed.at[par], landed.at[par], recv_sem.at[par]).wait()

    arrived(0)
    spread(landed.at[0], wide, x, y)

    @pl.loop(0, stations)
    def _(j):
        for part in range(2):
            partial[j, part] = product(j, part)

    arrived(1)
    spread(landed.at[1], wide, x, y)

    def owner(turn):
        return lax.rem(my_stn + jnp.where(turn < 2, 2 + turn, 3 - turn), stations)

    def send(j, part):
        source, landing = rows_out.at[j, part], v_ref.at[my_stn, part]

        @pl.when(j == my_stn)
        def _():
            pltpu.make_async_copy(source, landing, row_recv).start()

        @pl.when(j != my_stn)
        def _():
            pltpu.make_async_remote_copy(
                src_ref=source,
                dst_ref=landing,
                send_sem=row_send,
                recv_sem=row_recv,
                device_id=(j, my_chan),
                device_id_type=pl.DeviceIdType.MESH,
            ).start()

    def finish(j, part):
        total = (partial[j, part] + product(j, part)) * scaling
        rows_out[j, part] = total.astype(rows_out.dtype)

    @pl.loop(0, stations)
    def _(turn):
        j = owner(turn)
        finish(j, 0)

        @pl.when(turn > 0)
        def _():
            send(owner(turn - 1), 1)

        finish(j, 1)
        send(j, 0)

    send(owner(stations - 1), 1)
    for i in range(inputs):
        others = inbox.at[i, pl.ds(0, lane_count - 1)]
        pltpu.make_async_copy(others, others, in_send.at[i]).wait()
    for par in range(2):
        others = landed.at[par, pl.ds(0, landed.shape[1] - slots_each)]
        pltpu.make_async_copy(others, others, send_sem.at[par]).wait()
    pltpu.make_async_copy(v_ref, v_ref, row_recv).wait()
    others = v_ref.at[pl.ds(0, stations - 1)]
    pltpu.make_async_copy(others, others, row_send).wait()


def correlate(voltages, fir_taps, spectra_count, scaling, stations, lane_count):
    rows_dev, fr, slots = voltages.shape
    phases = fir_taps.shape[0]
    inputs = rows_dev // lane_count
    frames = lane_count // phases * fr
    half = slots // 2
    rows = inputs * frames
    parts = rows // LANES
    spans = slots // AVG
    whole = pl.BlockSpec(memory_space=pltpu.VMEM)
    whole_inputs = stations * rows_dev
    depth = AVG // 2 * LANES
    table = np.stack([dft_table(slots, par) for par in range(2)])
    twist = jnp.stack([first_twist(slots, phases, par) for par in range(2)])
    return pl.pallas_call(
        lambda *refs: channelise_kernel(spectra_count, scaling, *refs),
        out_shape=jax.ShapeDtypeStruct((stations, 2, rows_dev, whole_inputs), jnp.bfloat16),
        in_specs=[pl.BlockSpec(memory_space=pl.ANY), whole, whole, whole],
        out_specs=pl.BlockSpec(memory_space=pl.ANY),
        scratch_shapes=[
            pltpu.VMEM((inputs, lane_count, fr, slots), jnp.bfloat16),
            pltpu.VMEM((slots // LANES, frames + 8, LANES), jnp.float32),
            pltpu.VMEM((2, phases, rows, slots), jnp.bfloat16),
            pltpu.VMEM((phases, 2, parts, half // 2, LANES), jnp.bfloat16),
            pltpu.VMEM((2, half // 2, LANES), jnp.float32),
            pltpu.VMEM((2, stations, spans, parts, AVG, LANES), jnp.bfloat16),
            pltpu.VMEM((2, stations * spans * parts, AVG, LANES), jnp.bfloat16),
            pltpu.VMEM((LANES * AVG // 2, LANES), jnp.float32),
            pltpu.VMEM((whole_inputs, depth), jnp.bfloat16),
            pltpu.VMEM((whole_inputs, depth), jnp.bfloat16),
            pltpu.VMEM((stations, 2, rows_dev, whole_inputs), jnp.float32),
            pltpu.VMEM((stations, 2, rows_dev, whole_inputs), jnp.bfloat16),
            pltpu.SemaphoreType.DMA((inputs,)),
            pltpu.SemaphoreType.DMA((inputs,)),
            pltpu.SemaphoreType.DMA((2,)),
            pltpu.SemaphoreType.DMA((2,)),
            pltpu.SemaphoreType.DMA,
            pltpu.SemaphoreType.DMA,
        ],
        compiler_params=pltpu.CompilerParams(vmem_limit_bytes=60 << 20, has_side_effects=True),
        cost_estimate=pl.CostEstimate(flops=30 * 10**9, bytes_accessed=20 << 20, transcendentals=0),
    )(voltages, fir_taps, jnp.asarray(table), twist)


def per_device(voltages, fir_taps):
    fr, slots = voltages.shape[2:]
    phases, taps, _ = fir_taps.shape
    lane_count = lax.axis_size("chan")
    stations = lax.axis_size("stn")
    spectra_count = lane_count // phases * fr - (taps - 1)
    scaling = 1.0 / (phases * slots * AVG * spectra_count)
    mine = correlate(voltages[:, 0], fir_taps, spectra_count, scaling, stations, lane_count)
    return mine.astype(jnp.float32)[:, None]


def solution(mesh):
    return jax.shard_map(
        per_device,
        mesh=mesh,
        in_specs=(P("stn", "chan", None, None), P()),
        out_specs=P(None, "chan", None, "stn", None),
        check_vma=False,
    )
```

```python
import math

import jax
import jax.numpy as jnp
import numpy as np
from jax import lax
from jax.experimental import pallas as pl
from jax.experimental.pallas import tpu as pltpu
from jax.sharding import PartitionSpec as P

AVG = 16
LANES = 128


def dft_table(slots, par):
    half = slots // 2
    q = 2 * np.arange(half, dtype=np.int64) + par
    turns = (q[:, None] * np.arange(half, dtype=np.int64)) % slots
    angles = turns.astype(np.float64) * (-2.0 * math.pi / slots)
    parts = np.stack([np.cos(angles), np.sin(angles)]).reshape(2, 2, half // 2, half)
    table = parts.transpose(1, 0, 2, 3).reshape(slots, half).astype(np.float32)
    upper = table.astype(jnp.bfloat16)
    lower = (table - upper.astype(np.float32)).astype(jnp.bfloat16)
    return np.concatenate([upper, lower], axis=1)


def first_twist(slots, phases, par):
    half = slots // 2
    q = 2 * jnp.arange(half, dtype=jnp.int32) + par
    q = jnp.broadcast_to(q[:, None], (half, LANES))
    angles = q.astype(jnp.float32) * jnp.float32(-2.0 * math.pi / (phases * slots))
    return jnp.stack([jnp.cos(angles), jnp.sin(angles)])


def transform(phase, at, g, tab_ref, t1_ref, br, tw):
    rows, half = g.shape[0], g.shape[1] // 2
    size = half // 2
    dims = (((1,), (1,)), ((), ()))

    @pl.when(phase == 0)
    def _():
        tw[0] = jnp.ones(tw.shape[1:], jnp.float32)
        tw[1] = jnp.zeros(tw.shape[1:], jnp.float32)

    def product(table, values):
        return lax.dot_general(table, values, dims, preferred_element_type=jnp.float32)

    upper, lower = g[:, :half], g[:, half:]
    both = (
        product(tab_ref[:, :half], upper)
        + product(tab_ref[:, half:], upper)
        + product(tab_ref[:, :half], lower)
    )
    cos, sin = tw[0], tw[1]
    for part in range(rows // LANES):
        re = both[:size, part * LANES : (part + 1) * LANES]
        im = both[size:, part * LANES : (part + 1) * LANES]
        br[phase, 0, part] = (re * cos - im * sin).astype(jnp.bfloat16)
        br[phase, 1, part] = (re * sin + im * cos).astype(jnp.bfloat16)
    first, second = t1_ref[0, pl.ds(at, size), :], t1_ref[1, pl.ds(at, size), :]
    tw[0] = cos * first - sin * second
    tw[1] = cos * second + sin * first


def bands(frames, br, o_ref, base, start, emit):
    phases, _, parts, half, _ = br.shape
    root = math.sqrt(0.5)
    tile = 16
    count = half // tile
    left = lax.broadcasted_iota(jnp.int32, (tile, LANES), 1) < frames

    def four(a, b, c, d):
        (ar, ai), (b_r, bi), (cr, ci), (dr, di) = a, b, c, d
        er, ei, fr_, fi = ar + cr, ai + ci, ar - cr, ai - ci
        gr, gi, hr, hi = b_r + dr, bi + di, b_r - dr, bi - di
        return ((er + gr, ei + gi), (fr_ + hi, fi - hr), (er - gr, ei - gi), (fr_ - hi, fi + hr))

    @pl.loop(0, count)
    def _(step):
        block = lax.rem(start + step, count)
        at = pl.multiple_of(block * tile, tile)
        for part in range(parts):
            b = [
                tuple(br[p, ri, part, pl.ds(at, tile), :].astype(jnp.float32) for ri in range(2))
                for p in range(8)
            ]
            even = four(b[0], b[2], b[4], b[6])
            odd = four(b[1], b[3], b[5], b[7])
            (o1r, o1i), (o2r, o2i), (o3r, o3i) = odd[1:]
            turned = (
                odd[0],
                ((o1r + o1i) * root, (o1i - o1r) * root),
                (o2i, -o2r),
                ((o3i - o3r) * root, (-o3r - o3i) * root),
            )
            for c in range(4):
                re = even[c][0] + turned[c][0]
                im = even[c][1] + turned[c][1]
                first = jnp.where(left, re, pltpu.roll(im, frames, 1)).reshape(2, 8, LANES)
                second = jnp.where(left, pltpu.roll(re, frames, 1), im).reshape(2, 8, LANES)
                both = jnp.concatenate([first, second], axis=1)
                o_ref[c, pl.ds((base + block) * 2, 2), part] = both.astype(jnp.bfloat16)

        @pl.when(step > 0)
        def _():
            emit(base + lax.rem(start + step + count - 1, count))

    emit(base + lax.rem(start + count - 1, count))


def spread(r_ref, wide, x, y):
    inputs, lanes = x.shape[0], LANES
    items = x.shape[1] // lanes
    sub = wide.shape[0] // items
    tiles = sub * items // AVG

    @pl.loop(0, inputs // sub)
    def _(block):
        row = pl.multiple_of(block * sub, sub)
        at = pl.multiple_of(block * tiles, tiles)
        wide[...] = r_ref[pl.ds(at, tiles)].astype(jnp.float32).reshape(sub * items, lanes)
        left = lax.broadcasted_iota(jnp.int32, (sub, lanes), 1) < lanes // 2
        for item in range(items):
            value = wide[pl.ds(item, sub, stride=items), :]
            turned = pltpu.roll(value, lanes // 2, 1)
            lane = item * lanes
            x[pl.ds(row, sub), lane : lane + lanes] = value.astype(jnp.bfloat16)
            y[pl.ds(row, sub), lane : lane + lanes] = jnp.where(left, turned, -turned).astype(jnp.bfloat16)


def channelise_kernel(
    spectra_count,
    scaling,
    volt_ref,
    fir_ref,
    tab_ref,
    t1_ref,
    v_ref,
    inbox,
    xs,
    g,
    br,
    tw,
    out,
    landed,
    wide,
    x,
    y,
    partial,
    rows_out,
    in_send,
    in_recv,
    send_sem,
    recv_sem,
    row_send,
    row_recv,
):
    inputs, lane_count, fr, slots = inbox.shape
    phases, taps, _ = fir_ref.shape
    groups = lane_count // phases
    frames = groups * fr
    half = slots // 2
    stations, spans = out.shape[1], out.shape[2]
    my_stn, my_chan = lax.axis_index("stn"), lax.axis_index("chan")
    me = my_stn * spans + my_chan

    for i in range(inputs):

        @pl.loop(0, lane_count)
        def _(shift):
            lane = lax.rem(my_chan + shift, lane_count)
            source, landing = volt_ref.at[lane * inputs + i], inbox.at[i, my_chan]

            @pl.when(shift == 0)
            def _():
                pltpu.make_async_copy(source, landing, in_recv.at[i]).start()

            @pl.when(shift != 0)
            def _():
                pltpu.make_async_remote_copy(
                    src_ref=source,
                    dst_ref=landing,
                    send_sem=in_send.at[i],
                    recv_sem=in_recv.at[i],
                    device_id=(my_stn, lane),
                    device_id_type=pl.DeviceIdType.MESH,
                ).start()

    xs[:, frames:, :] = jnp.zeros((slots // LANES, xs.shape[1] - frames, LANES), jnp.float32)
    keep = lax.broadcasted_iota(jnp.int32, (frames, LANES), 0) < spectra_count

    @pl.loop(0, inputs)
    def _(i):
        pltpu.make_async_copy(inbox.at[i], inbox.at[i], in_recv.at[i]).wait()
        row = pl.multiple_of(i * frames, frames)

        @pl.loop(0, phases)
        def _(phase):
            for grp in range(groups):
                line = inbox[i, grp * phases + phase].astype(jnp.float32)
                for col in range(slots // LANES):
                    xs[col, grp * fr : (grp + 1) * fr, :] = line[:, col * LANES : (col + 1) * LANES]

            for chunk in range(half // LANES):

                def fir(at):
                    total = None
                    for k in range(taps):
                        term = fir_ref[phase, k : k + 1, at : at + LANES] * xs[
                            at // LANES, taps - 1 - k : taps - 1 - k + frames, :
                        ]
                        total = term if total is None else total + term
                    return jnp.where(keep, total, 0.0)

                at = chunk * LANES
                low, high = fir(at), fir(at + half)
                for par, value in ((0, low + high), (1, low - high)):
                    upper = value.astype(jnp.bfloat16)
                    lower = (value - upper.astype(jnp.float32)).astype(jnp.bfloat16)
                    g[par, phase, pl.ds(row, frames), at : at + LANES] = upper
                    g[par, phase, pl.ds(row, frames), half + at : half + at + LANES] = lower

    slots_each = landed.shape[1] // (stations * spans)

    def emit(par):
        def blocks(block):
            for turn in range(2):
                u = 2 * block + lax.rem(my_chan + turn, 2)
                for shift in range(stations):
                    c = lax.rem(my_stn + shift, stations)
                    source = out.at[par, c, u]
                    landing = landed.at[par, pl.ds(me * slots_each, slots_each)]
                    mine = jnp.logical_and(shift == 0, u == my_chan)

                    @pl.when(mine)
                    def _():
                        pltpu.make_async_copy(source, landing, recv_sem.at[par]).start()

                    @pl.when(jnp.logical_not(mine))
                    def _():
                        pltpu.make_async_remote_copy(
                            src_ref=source,
                            dst_ref=landing,
                            send_sem=send_sem.at[par],
                            recv_sem=recv_sem.at[par],
                            device_id=(c, u),
                            device_id_type=pl.DeviceIdType.MESH,
                        ).start()

        return blocks

    size = half // 2
    count = size // AVG
    own_half = my_chan // (spans // 2)
    for par in range(2):
        for turn in range(2):
            which = lax.rem(own_half + turn, 2)
            at = pl.multiple_of(which * size, size)
            table = tab_ref.at[par, pl.ds(pl.multiple_of(which * half, half), half)]

            @pl.loop(0, phases)
            def _(phase):
                transform(phase, at, g.at[par, phase], table, t1_ref.at[par], br, tw)

            bands(frames, br, out.at[par], which * count, lax.rem(my_chan // 2, count), emit(par))

    dims = (((1,), (1,)), ((), ()))
    height = rows_out.shape[2]

    def product(j, part):
        source = (x, y)[part]
        at = pl.multiple_of(j * height, height)
        return lax.dot_general(source[pl.ds(at, height), :], x[...], dims, preferred_element_type=jnp.float32)

    def arrived(par):
        pltpu.make_async_copy(landed.at[par], landed.at[par], recv_sem.at[par]).wait()

    arrived(0)
    spread(landed.at[0], wide, x, y)

    @pl.loop(0, stations)
    def _(j):
        for part in range(2):
            partial[j, part] = product(j, part)

    arrived(1)
    spread(landed.at[1], wide, x, y)

    def owner(turn):
        return lax.rem(my_stn + jnp.where(turn < 2, 2 + turn, 3 - turn), stations)

    def columns(j):
        return pl.ds(pl.multiple_of(j * height, height), height)

    def send(j, part):
        def copies(fly):
            lines = pl.ds(pl.multiple_of((2 * my_stn + part) * height, height), height)
            if part == 0:
                fly(rows_out.at[j, 0], v_ref.at[lines])
            else:
                for turn in range(1, stations):
                    other = columns(lax.rem(j + turn, stations))
                    fly(rows_out.at[j, 1, :, other], v_ref.at[lines, other])

        @pl.when(j == my_stn)
        def _():
            copies(lambda source, landing: pltpu.make_async_copy(source, landing, row_recv).start())

        @pl.when(j != my_stn)
        def _():
            copies(
                lambda source, landing: pltpu.make_async_remote_copy(
                    src_ref=source,
                    dst_ref=landing,
                    send_sem=row_send,
                    recv_sem=row_recv,
                    device_id=(j, my_chan),
                    device_id_type=pl.DeviceIdType.MESH,
                ).start()
            )

    def finish(j, part):
        total = (partial[j, part] + product(j, part)) * scaling
        rows_out[j, part] = total.astype(rows_out.dtype)
        if part == 1:
            row = lax.broadcasted_iota(jnp.int32, (height, height), 0)
            col = lax.broadcasted_iota(jnp.int32, (height, height), 1)
            both = [rows_out[j, p, :, columns(j)].astype(jnp.float32) for p in range(2)]
            rows_out[j, 0, :, columns(j)] = jnp.where(row <= col, both[0], both[1]).astype(rows_out.dtype)

    @pl.loop(0, stations)
    def _(turn):
        j = owner(turn)
        finish(j, 0)

        @pl.when(turn > 0)
        def _():
            send(owner(turn - 1), 1)

        finish(j, 1)
        send(j, 0)

    send(owner(stations - 1), 1)
    for i in range(inputs):
        others = inbox.at[i, pl.ds(0, lane_count - 1)]
        pltpu.make_async_copy(others, others, in_send.at[i]).wait()
    for par in range(2):
        others = landed.at[par, pl.ds(0, landed.shape[1] - slots_each)]
        pltpu.make_async_copy(others, others, send_sem.at[par]).wait()
    each = 2 * height - height // stations
    for sem, count in ((row_recv, stations), (row_send, stations - 1)):
        all_of = v_ref.at[pl.ds(0, count * each)]
        pltpu.make_async_copy(all_of, all_of, sem).wait()


def mirror_kernel(r_ref, o_ref):
    height = r_ref.shape[0] // 2
    j = lax.axis_index("stn")
    at = pl.ds(pl.multiple_of(j * height, height), height)
    for part in range(2):
        o_ref[0, 0, part] = r_ref[part * height : (part + 1) * height].astype(jnp.float32)
    row = lax.broadcasted_iota(jnp.int32, (height, height), 0)
    col = lax.broadcasted_iota(jnp.int32, (height, height), 1)
    both = r_ref[:height, at].astype(jnp.float32)
    turned = both.T
    o_ref[0, 0, 0, :, at] = jnp.where(row <= col, both, turned)
    o_ref[0, 0, 1, :, at] = jnp.where(row > col, both, jnp.where(row < col, -turned, 0.0))


def mirror(rows, stations):
    height = rows.shape[0] // stations // 2
    return pl.pallas_call(
        mirror_kernel,
        grid=(stations,),
        out_shape=jax.ShapeDtypeStruct((stations, 1, 2, height, rows.shape[1]), jnp.float32),
        in_specs=[pl.BlockSpec((2 * height, rows.shape[1]), lambda c: (c, 0))],
        out_specs=pl.BlockSpec((1, 1, 2, height, rows.shape[1]), lambda c: (c, 0, 0, 0, 0)),
    )(rows)


def correlate(voltages, fir_taps, spectra_count, scaling, stations, lane_count):
    rows_dev, fr, slots = voltages.shape
    phases = fir_taps.shape[0]
    inputs = rows_dev // lane_count
    frames = lane_count // phases * fr
    half = slots // 2
    rows = inputs * frames
    parts = rows // LANES
    spans = slots // AVG
    whole = pl.BlockSpec(memory_space=pltpu.VMEM)
    whole_inputs = stations * rows_dev
    depth = AVG // 2 * LANES
    table = np.stack([dft_table(slots, par) for par in range(2)])
    twist = jnp.stack([first_twist(slots, phases, par) for par in range(2)])
    return pl.pallas_call(
        lambda *refs: channelise_kernel(spectra_count, scaling, *refs),
        out_shape=jax.ShapeDtypeStruct((stations * 2 * rows_dev, whole_inputs), jnp.bfloat16),
        in_specs=[pl.BlockSpec(memory_space=pl.ANY), whole, whole, whole],
        out_specs=pl.BlockSpec(memory_space=pl.ANY),
        scratch_shapes=[
            pltpu.VMEM((inputs, lane_count, fr, slots), jnp.bfloat16),
            pltpu.VMEM((slots // LANES, frames + 8, LANES), jnp.float32),
            pltpu.VMEM((2, phases, rows, slots), jnp.bfloat16),
            pltpu.VMEM((phases, 2, parts, half // 2, LANES), jnp.bfloat16),
            pltpu.VMEM((2, half // 2, LANES), jnp.float32),
            pltpu.VMEM((2, stations, spans, parts, AVG, LANES), jnp.bfloat16),
            pltpu.VMEM((2, stations * spans * parts, AVG, LANES), jnp.bfloat16),
            pltpu.VMEM((LANES * AVG // 2, LANES), jnp.float32),
            pltpu.VMEM((whole_inputs, depth), jnp.bfloat16),
            pltpu.VMEM((whole_inputs, depth), jnp.bfloat16),
            pltpu.VMEM((stations, 2, rows_dev, whole_inputs), jnp.float32),
            pltpu.VMEM((stations, 2, rows_dev, whole_inputs), jnp.bfloat16),
            pltpu.SemaphoreType.DMA((inputs,)),
            pltpu.SemaphoreType.DMA((inputs,)),
            pltpu.SemaphoreType.DMA((2,)),
            pltpu.SemaphoreType.DMA((2,)),
            pltpu.SemaphoreType.DMA,
            pltpu.SemaphoreType.DMA,
        ],
        compiler_params=pltpu.CompilerParams(vmem_limit_bytes=60 << 20, has_side_effects=True),
        cost_estimate=pl.CostEstimate(flops=30 * 10**9, bytes_accessed=20 << 20, transcendentals=0),
    )(voltages, fir_taps, jnp.asarray(table), twist)


def per_device(voltages, fir_taps):
    fr, slots = voltages.shape[2:]
    phases, taps, _ = fir_taps.shape
    lane_count = lax.axis_size("chan")
    stations = lax.axis_size("stn")
    spectra_count = lane_count // phases * fr - (taps - 1)
    scaling = 1.0 / (phases * slots * AVG * spectra_count)
    mine = correlate(voltages[:, 0], fir_taps, spectra_count, scaling, stations, lane_count)
    return mirror(mine, stations)


def solution(mesh):
    return jax.shard_map(
        per_device,
        mesh=mesh,
        in_specs=(P("stn", "chan", None, None), P()),
        out_specs=P(None, "chan", None, "stn", None),
        check_vma=False,
    )
```

```python
import math

import jax
import jax.numpy as jnp
import numpy as np
from jax import lax
from jax.experimental import pallas as pl
from jax.experimental.pallas import tpu as pltpu
from jax.sharding import PartitionSpec as P

AVG = 16
LANES = 128


def dft_table(slots, par):
    half = slots // 2
    q = 2 * np.arange(half, dtype=np.int64) + par
    turns = (q[:, None] * np.arange(half, dtype=np.int64)) % slots
    angles = turns.astype(np.float64) * (-2.0 * math.pi / slots)
    parts = np.stack([np.cos(angles), np.sin(angles)]).reshape(2, 2, half // 2, half)
    table = parts.transpose(1, 0, 2, 3).reshape(slots, half).astype(np.float32)
    upper = table.astype(jnp.bfloat16)
    lower = (table - upper.astype(np.float32)).astype(jnp.bfloat16)
    return np.concatenate([upper, lower], axis=1)


def first_twist(slots, phases, par):
    half = slots // 2
    q = 2 * np.arange(half, dtype=np.float64) + par
    angles = np.broadcast_to(q[:, None], (half, LANES)) * (-2.0 * math.pi / (phases * slots))
    return np.stack([np.cos(angles), np.sin(angles)]).astype(np.float32)


def transform(phase, at, g, tab_ref, t1_ref, br, tw):
    rows, half = g.shape[0], g.shape[1] // 2
    size = half // 2
    dims = (((1,), (1,)), ((), ()))

    @pl.when(phase == 0)
    def _():
        tw[0] = jnp.ones(tw.shape[1:], jnp.float32)
        tw[1] = jnp.zeros(tw.shape[1:], jnp.float32)

    def product(table, values):
        return lax.dot_general(table, values, dims, preferred_element_type=jnp.float32)

    upper, lower = g[:, :half], g[:, half:]
    both = (
        product(tab_ref[:, :half], upper)
        + product(tab_ref[:, half:], upper)
        + product(tab_ref[:, :half], lower)
    )
    cos, sin = tw[0], tw[1]
    for part in range(rows // LANES):
        re = both[:size, part * LANES : (part + 1) * LANES]
        im = both[size:, part * LANES : (part + 1) * LANES]
        br[phase, 0, part] = (re * cos - im * sin).astype(jnp.bfloat16)
        br[phase, 1, part] = (re * sin + im * cos).astype(jnp.bfloat16)
    first, second = t1_ref[0, pl.ds(at, size), :], t1_ref[1, pl.ds(at, size), :]
    tw[0] = cos * first - sin * second
    tw[1] = cos * second + sin * first


def bands(frames, br, o_ref, base, start, emit):
    phases, _, parts, half, _ = br.shape
    root = math.sqrt(0.5)
    tile = 16
    count = half // tile
    left = lax.broadcasted_iota(jnp.int32, (tile, LANES), 1) < frames

    def four(a, b, c, d):
        (ar, ai), (b_r, bi), (cr, ci), (dr, di) = a, b, c, d
        er, ei, fr_, fi = ar + cr, ai + ci, ar - cr, ai - ci
        gr, gi, hr, hi = b_r + dr, bi + di, b_r - dr, bi - di
        return ((er + gr, ei + gi), (fr_ + hi, fi - hr), (er - gr, ei - gi), (fr_ - hi, fi + hr))

    @pl.loop(0, count)
    def _(step):
        block = lax.rem(start + step, count)
        at = pl.multiple_of(block * tile, tile)
        for part in range(parts):
            b = [
                tuple(br[p, ri, part, pl.ds(at, tile), :].astype(jnp.float32) for ri in range(2))
                for p in range(8)
            ]
            even = four(b[0], b[2], b[4], b[6])
            odd = four(b[1], b[3], b[5], b[7])
            (o1r, o1i), (o2r, o2i), (o3r, o3i) = odd[1:]
            turned = (
                odd[0],
                ((o1r + o1i) * root, (o1i - o1r) * root),
                (o2i, -o2r),
                ((o3i - o3r) * root, (-o3r - o3i) * root),
            )
            for c in range(4):
                re = even[c][0] + turned[c][0]
                im = even[c][1] + turned[c][1]
                first = jnp.where(left, re, pltpu.roll(im, frames, 1)).reshape(2, 8, LANES)
                second = jnp.where(left, pltpu.roll(re, frames, 1), im).reshape(2, 8, LANES)
                both = jnp.concatenate([first, second], axis=1)
                o_ref[c, pl.ds((base + block) * 2, 2), part] = both.astype(jnp.bfloat16)

        @pl.when(step > 0)
        def _():
            emit(base + lax.rem(start + step + count - 1, count))

    emit(base + lax.rem(start + count - 1, count))


def spread(r_ref, wide, x, y):
    inputs, lanes = x.shape[0], LANES
    items = x.shape[1] // lanes
    sub = wide.shape[0] // items
    tiles = sub * items // AVG

    @pl.loop(0, inputs // sub)
    def _(block):
        row = pl.multiple_of(block * sub, sub)
        at = pl.multiple_of(block * tiles, tiles)
        wide[...] = r_ref[pl.ds(at, tiles)].astype(jnp.float32).reshape(sub * items, lanes)
        left = lax.broadcasted_iota(jnp.int32, (sub, lanes), 1) < lanes // 2
        for item in range(items):
            value = wide[pl.ds(item, sub, stride=items), :]
            turned = pltpu.roll(value, lanes // 2, 1)
            lane = item * lanes
            x[pl.ds(row, sub), lane : lane + lanes] = value.astype(jnp.bfloat16)
            y[pl.ds(row, sub), lane : lane + lanes] = jnp.where(left, turned, -turned).astype(jnp.bfloat16)


def channelise_kernel(
    spectra_count,
    scaling,
    volt_ref,
    fir_ref,
    tab_ref,
    t1_ref,
    v_ref,
    inbox,
    xs,
    g,
    br,
    tw,
    out,
    landed,
    wide,
    x,
    y,
    partial,
    rows_out,
    in_send,
    in_recv,
    send_sem,
    recv_sem,
    row_send,
    row_recv,
):
    inputs, lane_count, fr, slots = inbox.shape
    phases, taps, _ = fir_ref.shape
    groups = lane_count // phases
    frames = groups * fr
    half = slots // 2
    stations, spans = out.shape[1], out.shape[2]
    my_stn, my_chan = lax.axis_index("stn"), lax.axis_index("chan")
    me = my_stn * spans + my_chan

    for i in range(inputs):

        @pl.loop(0, lane_count)
        def _(shift):
            lane = lax.rem(my_chan + shift, lane_count)
            source, landing = volt_ref.at[lane * inputs + i], inbox.at[i, my_chan]

            @pl.when(shift == 0)
            def _():
                pltpu.make_async_copy(source, landing, in_recv.at[i]).start()

            @pl.when(shift != 0)
            def _():
                pltpu.make_async_remote_copy(
                    src_ref=source,
                    dst_ref=landing,
                    send_sem=in_send.at[i],
                    recv_sem=in_recv.at[i],
                    device_id=(my_stn, lane),
                    device_id_type=pl.DeviceIdType.MESH,
                ).start()

    xs[:, frames:, :] = jnp.zeros((slots // LANES, xs.shape[1] - frames, LANES), jnp.float32)
    keep = lax.broadcasted_iota(jnp.int32, (frames, LANES), 0) < spectra_count

    @pl.loop(0, inputs)
    def _(i):
        pltpu.make_async_copy(inbox.at[i], inbox.at[i], in_recv.at[i]).wait()
        row = pl.multiple_of(i * frames, frames)

        @pl.loop(0, phases)
        def _(phase):
            for grp in range(groups):
                line = inbox[i, grp * phases + phase].astype(jnp.float32)
                for col in range(slots // LANES):
                    xs[col, grp * fr : (grp + 1) * fr, :] = line[:, col * LANES : (col + 1) * LANES]

            for chunk in range(half // LANES):

                def fir(at):
                    total = None
                    for k in range(taps):
                        term = fir_ref[phase, k : k + 1, at : at + LANES] * xs[
                            at // LANES, taps - 1 - k : taps - 1 - k + frames, :
                        ]
                        total = term if total is None else total + term
                    return jnp.where(keep, total, 0.0)

                at = chunk * LANES
                low, high = fir(at), fir(at + half)
                for par, value in ((0, low + high), (1, low - high)):
                    upper = value.astype(jnp.bfloat16)
                    lower = (value - upper.astype(jnp.float32)).astype(jnp.bfloat16)
                    g[par, phase, pl.ds(row, frames), at : at + LANES] = upper
                    g[par, phase, pl.ds(row, frames), half + at : half + at + LANES] = lower

    slots_each = landed.shape[1] // (stations * spans)

    def emit(par):
        def blocks(block):
            for turn in range(2):
                u = 2 * block + lax.rem(my_chan + turn, 2)
                for shift in range(stations):
                    c = lax.rem(my_stn + shift, stations)
                    source = out.at[par, c, u]
                    landing = landed.at[par, pl.ds(me * slots_each, slots_each)]
                    mine = jnp.logical_and(shift == 0, u == my_chan)

                    @pl.when(mine)
                    def _():
                        pltpu.make_async_copy(source, landing, recv_sem.at[par]).start()

                    @pl.when(jnp.logical_not(mine))
                    def _():
                        pltpu.make_async_remote_copy(
                            src_ref=source,
                            dst_ref=landing,
                            send_sem=send_sem.at[par],
                            recv_sem=recv_sem.at[par],
                            device_id=(c, u),
                            device_id_type=pl.DeviceIdType.MESH,
                        ).start()

        return blocks

    size = half // 2
    count = size // AVG
    own_half = my_chan // (spans // 2)
    for par in range(2):
        for turn in range(2):
            which = lax.rem(own_half + turn, 2)
            at = pl.multiple_of(which * size, size)
            table = tab_ref.at[par, pl.ds(pl.multiple_of(which * half, half), half)]

            @pl.loop(0, phases)
            def _(phase):
                transform(phase, at, g.at[par, phase], table, t1_ref.at[par], br, tw)

            bands(frames, br, out.at[par], which * count, lax.rem(my_chan // 2, count), emit(par))

    dims = (((1,), (1,)), ((), ()))
    height = rows_out.shape[2]

    def product(j, part):
        source = (x, y)[part]
        at = pl.multiple_of(j * height, height)
        return lax.dot_general(source[pl.ds(at, height), :], x[...], dims, preferred_element_type=jnp.float32)

    def arrived(par):
        pltpu.make_async_copy(landed.at[par], landed.at[par], recv_sem.at[par]).wait()

    arrived(0)
    spread(landed.at[0], wide, x, y)

    @pl.loop(0, stations)
    def _(j):
        for part in range(2):
            partial[j, part] = product(j, part)

    arrived(1)
    spread(landed.at[1], wide, x, y)

    def owner(turn):
        return lax.rem(my_stn + jnp.where(turn < 2, 2 + turn, 3 - turn), stations)

    def columns(j):
        return pl.ds(pl.multiple_of(j * height, height), height)

    def send(j, part):
        def copies(fly):
            lines = pl.ds(pl.multiple_of((2 * my_stn + part) * height, height), height)
            if part == 0:
                fly(rows_out.at[j, 0], v_ref.at[lines])
            else:
                for turn in range(1, stations):
                    other = columns(lax.rem(j + turn, stations))
                    fly(rows_out.at[j, 1, :, other], v_ref.at[lines, other])

        @pl.when(j == my_stn)
        def _():
            copies(lambda source, landing: pltpu.make_async_copy(source, landing, row_recv).start())

        @pl.when(j != my_stn)
        def _():
            copies(
                lambda source, landing: pltpu.make_async_remote_copy(
                    src_ref=source,
                    dst_ref=landing,
                    send_sem=row_send,
                    recv_sem=row_recv,
                    device_id=(j, my_chan),
                    device_id_type=pl.DeviceIdType.MESH,
                ).start()
            )

    def finish(j, part):
        total = (partial[j, part] + product(j, part)) * scaling
        rows_out[j, part] = total.astype(rows_out.dtype)
        if part == 1:
            row = lax.broadcasted_iota(jnp.int32, (height, height), 0)
            col = lax.broadcasted_iota(jnp.int32, (height, height), 1)
            both = [rows_out[j, p, :, columns(j)].astype(jnp.float32) for p in range(2)]
            rows_out[j, 0, :, columns(j)] = jnp.where(row <= col, both[0], both[1]).astype(rows_out.dtype)

    @pl.loop(0, stations)
    def _(turn):
        j = owner(turn)
        finish(j, 0)

        @pl.when(turn > 0)
        def _():
            send(owner(turn - 1), 1)

        finish(j, 1)
        send(j, 0)

    send(owner(stations - 1), 1)
    for i in range(inputs):
        others = inbox.at[i, pl.ds(0, lane_count - 1)]
        pltpu.make_async_copy(others, others, in_send.at[i]).wait()
    for par in range(2):
        others = landed.at[par, pl.ds(0, landed.shape[1] - slots_each)]
        pltpu.make_async_copy(others, others, send_sem.at[par]).wait()
    each = 2 * height - height // stations
    for sem, count in ((row_recv, stations), (row_send, stations - 1)):
        all_of = v_ref.at[pl.ds(0, count * each)]
        pltpu.make_async_copy(all_of, all_of, sem).wait()


def mirror_kernel(r_ref, o_ref):
    height = r_ref.shape[0] // 2
    j = lax.axis_index("stn")
    at = pl.ds(pl.multiple_of(j * height, height), height)
    for part in range(2):
        o_ref[0, 0, part] = r_ref[part * height : (part + 1) * height].astype(jnp.float32)
    row = lax.broadcasted_iota(jnp.int32, (height, height), 0)
    col = lax.broadcasted_iota(jnp.int32, (height, height), 1)
    both = r_ref[:height, at].astype(jnp.float32)
    turned = both.T
    o_ref[0, 0, 0, :, at] = jnp.where(row <= col, both, turned)
    o_ref[0, 0, 1, :, at] = jnp.where(row > col, both, jnp.where(row < col, -turned, 0.0))


def mirror(rows, stations):
    height = rows.shape[0] // stations // 2
    return pl.pallas_call(
        mirror_kernel,
        grid=(stations,),
        out_shape=jax.ShapeDtypeStruct((stations, 1, 2, height, rows.shape[1]), jnp.float32),
        in_specs=[pl.BlockSpec((2 * height, rows.shape[1]), lambda c: (c, 0))],
        out_specs=pl.BlockSpec((1, 1, 2, height, rows.shape[1]), lambda c: (c, 0, 0, 0, 0)),
    )(rows)


def correlate(voltages, fir_taps, spectra_count, scaling, stations, lane_count):
    rows_dev, fr, slots = voltages.shape
    phases = fir_taps.shape[0]
    inputs = rows_dev // lane_count
    frames = lane_count // phases * fr
    half = slots // 2
    rows = inputs * frames
    parts = rows // LANES
    spans = slots // AVG
    whole = pl.BlockSpec(memory_space=pltpu.VMEM)
    whole_inputs = stations * rows_dev
    depth = AVG // 2 * LANES
    table = np.stack([dft_table(slots, par) for par in range(2)])
    twist = np.stack([first_twist(slots, phases, par) for par in range(2)])
    return pl.pallas_call(
        lambda *refs: channelise_kernel(spectra_count, scaling, *refs),
        out_shape=jax.ShapeDtypeStruct((stations * 2 * rows_dev, whole_inputs), jnp.bfloat16),
        in_specs=[pl.BlockSpec(memory_space=pl.ANY), whole, whole, whole],
        out_specs=pl.BlockSpec(memory_space=pl.ANY),
        scratch_shapes=[
            pltpu.VMEM((inputs, lane_count, fr, slots), jnp.bfloat16),
            pltpu.VMEM((slots // LANES, frames + 8, LANES), jnp.float32),
            pltpu.VMEM((2, phases, rows, slots), jnp.bfloat16),
            pltpu.VMEM((phases, 2, parts, half // 2, LANES), jnp.bfloat16),
            pltpu.VMEM((2, half // 2, LANES), jnp.float32),
            pltpu.VMEM((2, stations, spans, parts, AVG, LANES), jnp.bfloat16),
            pltpu.VMEM((2, stations * spans * parts, AVG, LANES), jnp.bfloat16),
            pltpu.VMEM((LANES * AVG // 2, LANES), jnp.float32),
            pltpu.VMEM((whole_inputs, depth), jnp.bfloat16),
            pltpu.VMEM((whole_inputs, depth), jnp.bfloat16),
            pltpu.VMEM((stations, 2, rows_dev, whole_inputs), jnp.float32),
            pltpu.VMEM((stations, 2, rows_dev, whole_inputs), jnp.bfloat16),
            pltpu.SemaphoreType.DMA((inputs,)),
            pltpu.SemaphoreType.DMA((inputs,)),
            pltpu.SemaphoreType.DMA((2,)),
            pltpu.SemaphoreType.DMA((2,)),
            pltpu.SemaphoreType.DMA,
            pltpu.SemaphoreType.DMA,
        ],
        compiler_params=pltpu.CompilerParams(vmem_limit_bytes=60 << 20, has_side_effects=True),
        cost_estimate=pl.CostEstimate(flops=30 * 10**9, bytes_accessed=20 << 20, transcendentals=0),
    )(voltages, fir_taps, jnp.asarray(table), jnp.asarray(twist))


def per_device(voltages, fir_taps):
    fr, slots = voltages.shape[2:]
    phases, taps, _ = fir_taps.shape
    lane_count = lax.axis_size("chan")
    stations = lax.axis_size("stn")
    spectra_count = lane_count // phases * fr - (taps - 1)
    scaling = 1.0 / (phases * slots * AVG * spectra_count)
    mine = correlate(voltages[:, 0], fir_taps, spectra_count, scaling, stations, lane_count)
    return mirror(mine, stations)


def solution(mesh):
    return jax.shard_map(
        per_device,
        mesh=mesh,
        in_specs=(P("stn", "chan", None, None), P()),
        out_specs=P(None, "chan", None, "stn", None),
        check_vma=False,
    )
```
